32 devices in a mesh: blk: 16 (over z, y, x), rep: 2 (over core).
Axes of the slice: x: 2, y: 2, z: 4, core: 2. Of those that a mesh axis runs over, the one named last changes fastest.
Arguments:
- fwd_in: bfloat16 [14336, 1024], P(('blk', 'rep')), may hold values from -6 to 6
- bwd_in: bfloat16 [14336, 1024], P(('blk', 'rep')), may hold values from -6 to 6
- cotangent: bfloat16 [14336, 1024], P(('blk', 'rep')), may hold values from -6 to 6
- w_in: bfloat16 [1024, 8192], P(None, 'blk'), may hold values from -0.1875 to 0.1875
- w_out: bfloat16 [8192, 1024], P('blk'), may hold values from -0.125 to 0.125
Outputs:
- forward_out: bfloat16 [14336, 1024], P(('blk', 'rep'))
- input_grad: bfloat16 [14336, 1024], P(('blk', 'rep'))
- in_grad: float32 [1024, 8192], P('rep', 'blk')
- down_grad: float32 [8192, 1024], P('blk', 'rep')
The draws below stay inside these ranges and needn't reach their ends.
All inputs are finite; a program needn't handle non-finite values.
Results may differ from the reference program's by a relative error of at most 0.0066.
Values may be sent and summed in bfloat16 or wider, within the bound.
No kernel may reach another device: no remote copies, remote signals or barrier semaphores. Data moves between devices by JAX's collectives and lax.ppermute only.
A program may use at most 128 MiB of HBM per device.

```python
import jax
import jax.numpy as jnp
from jax import lax

D = 1024
HID_DEV = 512
TICKS = 4
MB_DEV = 448
FF = 8192
ROWS = 14336
N_BLK = 16
N_REP = 2


def steps_of(rng, extent, pieces, smallest, high):
    def one(dim, blocks):
        steps = jax.random.uniform(jax.random.fold_in(jax.random.fold_in(rng, 6), dim), (blocks,), jnp.float32, smallest / len(pieces), high / len(pieces))
        return jnp.repeat(jnp.exp(steps), extent[dim] // blocks).reshape((-1,) + (1,) * (len(extent) - dim - 1))

    loudness = one(*pieces[0])
    for cut in pieces[1:]:
        loudness = loudness * one(*cut)
    return loudness


def noise(key, dims, scale, reach, split=(), kind=jnp.bfloat16):
    result = jax.random.normal(key, dims, jnp.float32) * scale
    if len(split) > 0:
        result = steps_of(key, dims, split, -0.22, 0.18) * result
    return jnp.clip(result, min=-reach, max=reach).astype(kind)


def setup_inputs(seed: int = 0) -> dict:
    key_list = jax.random.split(jax.random.key(seed), 6)
    return {
        "fwd_in": noise(key_list[0], (ROWS, D), 1.0, 6.0, ((0, 32),)),
        "bwd_in": noise(key_list[1], (ROWS, D), 1.0, 6.0, ((0, 32),)),
        "cotangent": noise(key_list[2], (ROWS, D), 1.0, 6.0, ((0, 32),)),
        "w_in": noise(key_list[3], (D, FF), D ** -0.5, 0.1875, ((1, 16),)),
        "w_out": noise(key_list[4], (FF, D), (TICKS * HID_DEV) ** -0.5, 0.125, ((0, 16),)),
    }


def inner(left, right, left_dim, right_dim):
    return lax.dot_general(left, right, (((left_dim,), (right_dim,)), ((), ())), preferred_element_type=jnp.float32)

def slot_pair(w_in, w_out, holder):
    offset = (holder * HID_DEV).astype(jnp.int32)
    return (lax.dynamic_slice_in_dim(w_in, offset, HID_DEV, 1), lax.dynamic_slice_in_dim(w_out, offset, HID_DEV, 0))

def backward_pieces(inputs, cotan, w_in_slot, w_out_slot):
    preact = jnp.dot(inputs, w_in_slot, preferred_element_type=jnp.float32)
    active, pullback = jax.vjp(jax.nn.gelu, preact)
    hidden = active.astype(jnp.bfloat16)
    hid_grad = inner(cotan, w_out_slot, 1, 1)
    pre_grad = pullback(hid_grad)[0].astype(jnp.bfloat16)
    return (hidden, pre_grad)

def reference(fwd_in, bwd_in, cotangent, w_in, w_out):
    span_rows = MB_DEV * N_REP

    def take_block(array, block):
        offset = (block * span_rows).astype(jnp.int32)
        return lax.dynamic_slice_in_dim(array, offset, span_rows, 0)

    def per_block(block):
        fwd_rows = take_block(fwd_in, block)
        bwd_rows = take_block(bwd_in, block)
        cot_rows = take_block(cotangent, block)
        fwd_sum = jnp.zeros((span_rows, D), jnp.float32)
        grad_sum = jnp.zeros((span_rows, D), jnp.float32)
        for tick in range(TICKS):
            holder = ((block + N_BLK - tick) % N_BLK).astype(jnp.int32)
            w_in_slot, w_out_slot = slot_pair(w_in, w_out, holder)
            preact = jnp.dot(fwd_rows, w_in_slot, preferred_element_type=jnp.float32)
            fwd_sum = fwd_sum + jnp.dot(jax.nn.gelu(preact).astype(jnp.bfloat16), w_out_slot, preferred_element_type=jnp.float32)
            hidden, pre_grad = backward_pieces(bwd_rows, cot_rows, w_in_slot, w_out_slot)
            grad_sum = grad_sum + inner(pre_grad, w_in_slot, 1, 1)
        return (fwd_sum.astype(jnp.bfloat16), grad_sum.astype(jnp.bfloat16))

    def per_holder(holder):
        w_in_slot, w_out_slot = slot_pair(w_in, w_out, holder)
        in_sum = jnp.zeros((D, HID_DEV), jnp.float32)
        out_sum = jnp.zeros((HID_DEV, D), jnp.float32)
        for tick in range(TICKS):
            block = ((holder + tick) % N_BLK).astype(jnp.int32)
            bwd_rows = take_block(bwd_in, block)
            cot_rows = take_block(cotangent, block)
            hidden, pre_grad = backward_pieces(bwd_rows, cot_rows, w_in_slot, w_out_slot)
            in_sum = in_sum + inner(bwd_rows, pre_grad, 0, 0)
            out_sum = out_sum + inner(hidden, cot_rows, 0, 0)
        return (in_sum, out_sum)
    blocks = jnp.arange(N_BLK, dtype=jnp.int32)
    fwd_parts, grad_parts = lax.map(per_block, blocks)
    in_parts, out_parts = lax.map(per_holder, blocks)
    forward_out = fwd_parts.reshape(-1, D)
    input_grad = grad_parts.reshape(-1, D)
    in_grad = jnp.transpose(in_parts, (1, 0, 2)).reshape(D, N_BLK * HID_DEV)
    down_grad = out_parts.reshape(N_BLK * HID_DEV, D)
    return (forward_out, input_grad, in_grad, down_grad)
```

```python
import jax
import jax.numpy as jnp
from jax import lax
from jax.sharding import PartitionSpec as P

TICKS = 4
SIDE = 2


def routes(n_blk, n_rep):
    groups = n_blk // TICKS
    across, beside, forward = [], [], []
    for blk in range(n_blk):
        group, place = blk // TICKS, blk % TICKS
        for rep in range(n_rep):
            source = blk * n_rep + rep

            def target(to):
                to_group = group + (1 if to < place else 0)
                return ((to_group % groups) * TICKS + to) * n_rep + rep

            beside.append((source, target(place ^ 1)))
            across.append((source, target(place ^ SIDE)))
            forward.append((source, (group * TICKS + (place ^ 1)) * n_rep + rep))
    return beside, across, forward


def back(pairs):
    return [(target, source) for source, target in pairs]


def inner(left, right, left_dim, right_dim):
    return lax.dot_general(
        left, right, (((left_dim,), (right_dim,)), ((), ())), preferred_element_type=jnp.float32
    )


def on_device(fwd_in, bwd_in, cotangent, w_in, w_out):
    axes = ("blk", "rep")
    n_blk, n_rep = lax.axis_size("blk"), lax.axis_size("rep")
    beside, across, forward = routes(n_blk, n_rep)
    rep = lax.axis_index("rep")
    width = w_in.shape[1] // n_rep
    rows = fwd_in.shape[0]
    span = w_in.shape[0] // n_rep
    swap = [(0, 1), (1, 0)]

    def move(value, pairs):
        return lax.ppermute(value, axes, pairs)

    def peer(value):
        return lax.ppermute(value, "rep", swap)

    wi = lax.dynamic_slice_in_dim(w_in, rep * width, width, 1)
    wo = lax.dynamic_slice_in_dim(w_out, rep * width, width, 0)
    xi, yi = move(wi, beside), move(wi, across)
    di = move(yi, forward)
    xo, yo = move(wo, beside), move(wo, across)
    do = move(yo, forward)

    fwd = jnp.concatenate([fwd_in, peer(fwd_in)], 0)
    bwd = jnp.concatenate([bwd_in, peer(bwd_in)], 0)
    cot = jnp.concatenate([cotangent, peer(cotangent)], 0)

    def slot(a, b):
        hid_f = jax.nn.gelu(jnp.dot(fwd, a, preferred_element_type=jnp.float32)).astype(jnp.bfloat16)
        out = jnp.dot(hid_f, b, preferred_element_type=jnp.float32)
        pre = jnp.dot(bwd, a, preferred_element_type=jnp.float32)
        active, pullback = jax.vjp(jax.nn.gelu, pre)
        hid = active.astype(jnp.bfloat16)
        down = inner(hid, cot, 0, 0)
        pre_grad = pullback(inner(cot, b, 1, 1))[0].astype(jnp.bfloat16)
        into = inner(bwd, pre_grad, 0, 0)
        grad = inner(pre_grad, a, 1, 1)
        return out, grad, into, down

    out_0, grad_0, into_0, down_0 = slot(wi, wo)
    out_x, grad_x, into_x, down_x = slot(xi, xo)
    out_y, grad_y, into_y, down_y = slot(yi, yo)
    out_d, grad_d, into_d, down_d = slot(di, do)

    def collect(own, g_x, g_y, g_d):
        g_y = g_y + move(g_d.astype(jnp.bfloat16), back(forward)).astype(jnp.float32)
        from_y = move(g_y.astype(jnp.bfloat16), back(across)).astype(jnp.float32)
        from_x = move(g_x.astype(jnp.bfloat16), back(beside)).astype(jnp.float32)
        return own + from_x + from_y

    def share(total, dim, out_dim):
        mine = lax.dynamic_slice_in_dim(total, rep * span, span, dim)
        other = peer(lax.dynamic_slice_in_dim(total, (1 - rep) * span, span, dim))
        return jnp.where(
            rep == 0,
            jnp.concatenate([mine, other], out_dim),
            jnp.concatenate([other, mine], out_dim),
        )

    down_grad = share(collect(down_0, down_x, down_y, down_d), 1, 0)
    in_grad = share(collect(into_0, into_x, into_y, into_d), 0, 1)

    def halves(parts):
        other = peer(sum(p[rows:] for p in parts).astype(jnp.bfloat16)).astype(jnp.float32)
        return (sum(p[:rows] for p in parts) + other).astype(jnp.bfloat16)

    forward_out = halves([out_0, out_x, out_y, out_d])
    input_grad = halves([grad_0, grad_x, grad_y, grad_d])
    return (forward_out, input_grad, in_grad, down_grad)


def solution(mesh):
    in_specs = (
        P(("blk", "rep"), None),
        P(("blk", "rep"), None),
        P(("blk", "rep"), None),
        P(None, "blk"),
        P("blk", None),
    )
    out_specs = (P(("blk", "rep"), None), P(("blk", "rep"), None), P("rep", "blk"), P("blk", "rep"))
    return jax.shard_map(
        on_device, mesh=mesh, in_specs=in_specs, out_specs=out_specs, check_vma=False
    )
```

```python
import functools

import jax
import jax.numpy as jnp
from jax import lax
from jax.experimental import pallas as pl
from jax.experimental.pallas import tpu as pltpu
from jax.sharding import PartitionSpec as P


TICKS = 4
SIDE = 2
ROOT = 0.7978845608028654
CUBE = 0.044715
F32, BF16 = jnp.float32, jnp.bfloat16


def routes(n_blk, n_rep):
    groups = n_blk // TICKS
    across, beside, returned, forward, third = [], [], [], [], []
    for blk in range(n_blk):
        group, place = blk // TICKS, blk % TICKS
        for rep in range(n_rep):
            source = blk * n_rep + rep

            def target(to):
                to_group = group + (1 if to < place else 0)
                return ((to_group % groups) * TICKS + to) * n_rep + rep

            returned.append((target(place ^ 1), source))
            if place < TICKS - 1:
                beside.append((source, target(place ^ 1)))
            if place == 0:
                third.append((source, (group * TICKS + SIDE) * n_rep + rep))
            across.append((source, target(place ^ SIDE)))
            forward.append((source, (group * TICKS + (place ^ 1)) * n_rep + rep))
    return beside, returned, across, forward, third


def back(pairs):
    return [(target, source) for source, target in pairs]


def mul(left, right, left_dim, right_dim):
    return lax.dot_general(
        left, right, (((left_dim,), (right_dim,)), ((), ())), preferred_element_type=F32
    )


def tanh_part(v):
    return jnp.tanh(ROOT * (v + CUBE * (v * v * v)))


def cut_kernel(dim, whole, part, sem):
    size = part.shape[dim]
    where = pl.ds(pl.multiple_of(lax.axis_index("rep") * size, size), size)
    copy = pltpu.make_async_copy(whole.at[:, where] if dim else whole.at[where, :], part, sem)
    copy.start()
    copy.wait()


def in_kernel(b0, b1, c0, c1, wi, down, slope, hid):
    for half, b in enumerate((b0, b1)):
        v = mul(b[...], wi[...], 1, 0)
        t = tanh_part(v)
        up = 0.5 * (1.0 + t)
        hid[half] = (v * up).astype(BF16)
        slope[half] = up + (0.5 * ROOT) * v * (1.0 - t * t) * (1.0 + (3.0 * CUBE) * (v * v))
    down[...] = (mul(hid[0], c0[...], 0, 0) + mul(hid[1], c1[...], 0, 0)).astype(down.dtype)


def out_kernel(b0, b1, c0, c1, wo, slope, into, pre):
    for half, c in enumerate((c0, c1)):
        pre[half] = (mul(c[...], wo[...], 1, 1) * slope[half]).astype(BF16)
    into[...] = (mul(pre[0], b0[...], 0, 0) + mul(pre[1], b1[...], 0, 0)).astype(into.dtype)


def fwd_kernel(f0, f1, wi, hid):
    for half, f in enumerate((f0, f1)):
        v = mul(f[...], wi[...], 1, 0)
        hid[half] = (v * (0.5 * (1.0 + tanh_part(v)))).astype(BF16)


def sum_kernel(dim, *refs):
    lefts, rights = refs[:TICKS], refs[TICKS : 2 * TICKS]
    give, keep, left, right = refs[2 * TICKS :]
    size = lefts[0].shape[2]
    for slot in range(TICKS):
        where = slice(slot * size, (slot + 1) * size)
        if dim:
            right[:, where] = rights[slot][...]
        else:
            right[where, :] = rights[slot][...]
        for half in range(2):
            left[half, :, where] = lefts[slot][half]
    give[...] = mul(left[1], right[...], 1, dim).astype(BF16)
    keep[...] = mul(left[0], right[...], 1, dim)


def add_kernel(a, b, out):
    out[...] = (a[...].astype(F32) + b[...].astype(F32)).astype(out.dtype)


def split_kernel(own, x, y, keep, give):
    rep, size = lax.axis_index("rep"), keep.shape[1]
    for out, at in ((give, 1 - rep), (keep, rep)):
        where = pl.ds(pl.multiple_of(at * size, size), size)
        out[...] = own[:, where] + x[:, where].astype(F32) + y[:, where].astype(F32)


def join_kernel(dim, keep, got, out):
    rep, size = lax.axis_index("rep"), keep.shape[0]
    for part, at in ((keep, rep), (got, 1 - rep)):
        where = pl.ds(pl.multiple_of(at * size, size), size)
        if dim:
            out[:, where] = part[...].T
        else:
            out[where, :] = part[...]


def call(body, outs, flops, *args, scratch=(), far=False):
    vmem = pl.BlockSpec(memory_space=pltpu.VMEM)
    moved = sum(a.size * a.dtype.itemsize for a in args)
    return pl.pallas_call(
        body,
        out_shape=outs,
        in_specs=[pl.BlockSpec(memory_space=pltpu.HBM) if far else vmem] * len(args),
        out_specs=jax.tree.map(lambda _: vmem, outs),
        scratch_shapes=list(scratch),
        compiler_params=pltpu.CompilerParams(vmem_limit_bytes=14 << 20),
        cost_estimate=pl.CostEstimate(flops=flops, bytes_accessed=moved, transcendentals=0),
    )(*args)


def window(fwd_in, bwd_in, cotangent, w_in, w_out):
    axes = ("blk", "rep")
    n_blk, n_rep = lax.axis_size("blk"), lax.axis_size("rep")
    beside, returned, across, forward, third = routes(n_blk, n_rep)
    width = w_in.shape[1] // n_rep
    rows, model = fwd_in.shape
    span = model // n_rep
    swap = [(0, 1), (1, 0)]
    unit = 2 * 2 * rows * model * width

    def move(value, pairs):
        return lax.ppermute(value, axes, pairs)

    def peer(value):
        return lax.ppermute(value, "rep", swap)

    shape = jax.ShapeDtypeStruct
    hidden = shape((2, rows, width), BF16)

    def run(body, outs, flops, *args, **rest):
        return call(body, outs, flops, *args, **rest)

    def in_part(a, kind):
        return run(
            in_kernel,
            (shape((width, model), kind), shape((2, rows, width), F32)),
            2 * unit,
            bwd_in, bwd_peer, cotangent, cot_peer, a,
            scratch=[pltpu.VMEM((2, rows, width), BF16)],
        )

    def out_part(b, slope, kind):
        return run(
            out_kernel,
            (shape((width, model), kind), hidden),
            2 * unit,
            bwd_in, bwd_peer, cotangent, cot_peer, b, slope,
        )

    def fwd_part(a):
        return run(fwd_kernel, hidden, unit, fwd_in, fwd_peer, a)

    def cut(whole, dim):
        size = (model, width) if dim else (width, model)
        return run(
            functools.partial(cut_kernel, dim), shape(size, BF16), unit // 4, whole,
            scratch=[pltpu.SemaphoreType.DMA], far=True,
        )

    def add(a, b):
        return run(add_kernel, shape(a.shape, BF16), unit // 4, a, b)

    wi, wo = cut(w_in, 1), cut(w_out, 0)
    yi, xi = move(wi, across), move(wi, beside)
    yo, xo = move(wo, across), move(wo, beside)
    bwd_peer, cot_peer, fwd_peer = peer(bwd_in), peer(cotangent), peer(fwd_in)
    di, do = move(yi, forward), move(yo, forward)
    xi = add(xi, move(di, third))
    xo = add(xo, move(do, third))

    down_0, slope_0 = in_part(wi, F32)
    into_0, pre_0 = out_part(wo, slope_0, F32)
    hid_0 = fwd_part(wi)
    down_y, slope_y = in_part(yi, BF16)
    into_y, pre_y = out_part(yo, slope_y, BF16)
    hid_y = fwd_part(yi)
    down_d, slope_d = in_part(di, BF16)
    into_d, pre_d = out_part(do, slope_d, BF16)
    hid_d = fwd_part(di)
    down_x, slope_x = in_part(xi, BF16)
    into_x, pre_x = out_part(xo, slope_x, BF16)
    hid_x = fwd_part(xi)

    down_y = add(down_y, move(down_d, back(forward)))
    into_y = add(into_y, move(into_d, back(forward)))
    down_across, into_across = move(down_y, back(across)), move(into_y, back(across))
    down_beside, into_beside = move(down_x, returned), move(into_x, returned)

    def sums(lefts, rights, dim):
        give, keep = run(
            functools.partial(sum_kernel, dim),
            (shape((rows, model), BF16), shape((rows, model), F32)),
            4 * unit, *lefts, *rights,
            scratch=[
                pltpu.VMEM((2, rows, TICKS * width), BF16),
                pltpu.VMEM((model, TICKS * width) if dim else (TICKS * width, model), BF16),
            ],
        )
        return add(keep, peer(give))

    forward_out = sums((hid_0, hid_x, hid_y, hid_d), (wo, xo, yo, do), 0)
    input_grad = sums((pre_0, pre_x, pre_y, pre_d), (wi, xi, yi, di), 1)

    def share(own, x, y, dim):
        half = shape((width, span), F32)
        keep, give = run(split_kernel, (half, half), unit // 4, own, x, y)
        size = (span, n_rep * width) if dim else (n_rep * width, span)
        return run(
            functools.partial(join_kernel, dim), shape(size, F32), unit // 4,
            keep, peer(give),
        )

    down_grad = share(down_0, down_beside, down_across, 0)
    in_grad = share(into_0, into_beside, into_across, 1)
    return (forward_out, input_grad, in_grad, down_grad)


def solution(mesh):
    in_specs = (
        P(("blk", "rep"), None),
        P(("blk", "rep"), None),
        P(("blk", "rep"), None),
        P(None, "blk"),
        P("blk", None),
    )
    out_specs = (P(("blk", "rep"), None), P(("blk", "rep"), None), P("rep", "blk"), P("blk", "rep"))
    return jax.shard_map(window, mesh=mesh, in_specs=in_specs, out_specs=out_specs, check_vma=False)
```

```python
import functools

import jax
import jax.numpy as jnp
from jax import lax
from jax.experimental import pallas as pl
from jax.experimental.pallas import tpu as pltpu
from jax.sharding import PartitionSpec as P


TICKS = 4
SIDE = 2
ROOT = 0.7978845608028654
CUBE = 0.044715
F32, BF16 = jnp.float32, jnp.bfloat16


WEIGHT_KINDS = {"i": "A", "o": "A"}
GRAD_KINDS = {"d": "B", "n": "B"}


def routes(n_blk, n_rep):
    groups = n_blk // TICKS
    names = ("across", "across_but", "beside", "beside_but_last", "side", "third", "turn", "over")
    pairs = {name: [] for name in names}
    for blk in range(n_blk):
        group, place = blk // TICKS, blk % TICKS
        for rep in range(n_rep):
            source = blk * n_rep + rep

            def at(to, later=0):
                return (((group + later) % groups) * TICKS + to) * n_rep + rep

            def add(name, to, later=0):
                pairs[name].append((source, at(to, later)))

            add("across", place ^ SIDE, place ^ SIDE < place)
            add("beside", place ^ 1, place ^ 1 < place)
            if place < TICKS - 1:
                add("beside_but_last", place ^ 1, place ^ 1 < place)
            add("side", place ^ 1)
            if place == 0:
                add("third", SIDE)
                add("over", 1)
            if place != SIDE:
                add("across_but", place ^ SIDE, place ^ SIDE < place)
            add("turn", place ^ SIDE, (place == TICKS - 1) - (place == 0))
    return pairs


def back(pairs):
    return [(target, source) for source, target in pairs]


def mul(left, right, left_dim, right_dim):
    return lax.dot_general(
        left, right, (((left_dim,), (right_dim,)), ((), ())), preferred_element_type=F32
    )


def tanh_part(v):
    return jnp.tanh(ROOT * (v + CUBE * (v * v * v)))


def cut_kernel(dim, whole, part, sem):
    size = part.shape[dim]
    where = pl.ds(pl.multiple_of(lax.axis_index("rep") * size, size), size)
    copy = pltpu.make_async_copy(whole.at[:, where] if dim else whole.at[where, :], part, sem)
    copy.start()
    copy.wait()


def in_kernel(b0, b1, c0, c1, wi, down, slope, hid):
    for half, b in enumerate((b0, b1)):
        v = mul(b[...], wi[...], 1, 0)
        t = tanh_part(v)
        up = 0.5 * (1.0 + t)
        hid[half] = (v * up).astype(BF16)
        slope[half] = up + (0.5 * ROOT) * v * (1.0 - t * t) * (1.0 + (3.0 * CUBE) * (v * v))
    down[...] = (mul(hid[0], c0[...], 0, 0) + mul(hid[1], c1[...], 0, 0)).astype(down.dtype)


def out_kernel(b0, b1, c0, c1, wo, slope, into, pre):
    for half, c in enumerate((c0, c1)):
        pre[half] = (mul(c[...], wo[...], 1, 1) * slope[half]).astype(BF16)
    into[...] = (mul(pre[0], b0[...], 0, 0) + mul(pre[1], b1[...], 0, 0)).astype(into.dtype)


def fwd_kernel(f0, f1, wi, hid):
    for half, f in enumerate((f0, f1)):
        v = mul(f[...], wi[...], 1, 0)
        hid[half] = (v * (0.5 * (1.0 + tanh_part(v)))).astype(BF16)


def sum_kernel(dim, *refs):
    lefts, rights = refs[:TICKS], refs[TICKS : 2 * TICKS]
    give, keep, left, right = refs[2 * TICKS :]
    size = lefts[0].shape[2]
    for slot in range(TICKS):
        where = slice(slot * size, (slot + 1) * size)
        if dim:
            right[:, where] = rights[slot][...]
        else:
            right[where, :] = rights[slot][...]
        for half in range(2):
            left[half, :, where] = lefts[slot][half]
    give[...] = mul(left[1], right[...], 1, dim).astype(BF16)
    keep[...] = mul(left[0], right[...], 1, dim)


def add_kernel(a, b, out):
    out[...] = (a[...].astype(F32) + b[...].astype(F32)).astype(out.dtype)


def split_kernel(own, x, y, keep, give):
    rep, size = lax.axis_index("rep"), keep.shape[1]
    for out, at in ((give, 1 - rep), (keep, rep)):
        where = pl.ds(pl.multiple_of(at * size, size), size)
        out[...] = own[:, where] + x[:, where].astype(F32) + y[:, where].astype(F32)


def join_kernel(dim, keep, got, out):
    rep, size = lax.axis_index("rep"), keep.shape[0]
    for part, at in ((keep, rep), (got, 1 - rep)):
        where = pl.ds(pl.multiple_of(at * size, size), size)
        if dim:
            out[:, where] = part[...].T
        else:
            out[where, :] = part[...]


def call(body, outs, flops, *args, scratch=(), far=False):
    vmem = pl.BlockSpec(memory_space=pltpu.VMEM)
    moved = sum(a.size * a.dtype.itemsize for a in args)
    return pl.pallas_call(
        body,
        out_shape=outs,
        in_specs=[pl.BlockSpec(memory_space=pltpu.HBM) if far else vmem] * len(args),
        out_specs=jax.tree.map(lambda _: vmem, outs),
        scratch_shapes=list(scratch),
        compiler_params=pltpu.CompilerParams(vmem_limit_bytes=14 << 20),
        cost_estimate=pl.CostEstimate(flops=flops, bytes_accessed=moved, transcendentals=0),
    )(*args)


def window(fwd_in, bwd_in, cotangent, w_in, w_out):
    axes = ("blk", "rep")
    n_blk, n_rep = lax.axis_size("blk"), lax.axis_size("rep")
    pairs = routes(n_blk, n_rep)
    width = w_in.shape[1] // n_rep
    rows, model = fwd_in.shape
    span = model // n_rep
    swap = [(0, 1), (1, 0)]
    unit = 2 * 2 * rows * model * width

    def move(value, pairs):
        return lax.ppermute(value, axes, pairs)

    def peer(value):
        return lax.ppermute(value, "rep", swap)

    shape = jax.ShapeDtypeStruct
    hidden = shape((2, rows, width), BF16)

    def run(body, outs, flops, *args, **rest):
        return call(body, outs, flops, *args, **rest)

    def in_part(a, kind):
        return run(
            in_kernel,
            (shape((width, model), kind), shape((2, rows, width), F32)),
            2 * unit,
            bwd_in, bwd_peer, cotangent, cot_peer, a,
            scratch=[pltpu.VMEM((2, rows, width), BF16)],
        )

    def out_part(b, slope, kind):
        return run(
            out_kernel,
            (shape((width, model), kind), hidden),
            2 * unit,
            bwd_in, bwd_peer, cotangent, cot_peer, b, slope,
        )

    def fwd_part(a):
        return run(fwd_kernel, hidden, unit, fwd_in, fwd_peer, a)

    def cut(whole, dim):
        size = (model, width) if dim else (width, model)
        return run(
            functools.partial(cut_kernel, dim), shape(size, BF16), unit // 4, whole,
            scratch=[pltpu.SemaphoreType.DMA], far=True,
        )

    def add(a, b):
        return run(add_kernel, shape(a.shape, BF16), unit // 4, a, b)

    def spread(label, weight):
        x = move(weight, pairs["beside"])
        y = move(weight, pairs["across"])
        if WEIGHT_KINDS[label] == "A":
            d = move(y, pairs["side"])
        else:
            d = move(x, pairs["turn"])
        return x, y, d

    wi, wo = cut(w_in, 1), cut(w_out, 0)
    xi, yi, di = spread("i", wi)
    xo, yo, do = spread("o", wo)
    bwd_peer, cot_peer, fwd_peer = peer(bwd_in), peer(cotangent), peer(fwd_in)

    down_0, slope_0 = in_part(wi, F32)
    into_0, pre_0 = out_part(wo, slope_0, F32)
    hid_0 = fwd_part(wi)
    down_y, slope_y = in_part(yi, BF16)
    into_y, pre_y = out_part(yo, slope_y, BF16)
    hid_y = fwd_part(yi)
    down_d, slope_d = in_part(di, BF16)
    into_d, pre_d = out_part(do, slope_d, BF16)
    hid_d = fwd_part(di)
    down_x, slope_x = in_part(xi, BF16)
    into_x, pre_x = out_part(xo, slope_x, BF16)
    hid_x = fwd_part(xi)

    def gather(label, g_x, g_y, g_d):
        rest = back(pairs["across"])
        if GRAD_KINDS[label] == "C":
            g_d = add(g_d, move(g_y, pairs["over"]))
            rest = back(pairs["across_but"])
        if GRAD_KINDS[label] == "A":
            g_y = add(g_y, move(g_d, back(pairs["side"])))
        else:
            g_x = add(g_x, move(g_d, back(pairs["turn"])))
        return (move(g_x, back(pairs["beside"])), move(g_y, rest))

    down_beside, down_across = gather("d", down_x, down_y, down_d)
    into_beside, into_across = gather("n", into_x, into_y, into_d)

    def sums(lefts, rights, dim):
        give, keep = run(
            functools.partial(sum_kernel, dim),
            (shape((rows, model), BF16), shape((rows, model), F32)),
            4 * unit, *lefts, *rights,
            scratch=[
                pltpu.VMEM((2, rows, TICKS * width), BF16),
                pltpu.VMEM((model, TICKS * width) if dim else (TICKS * width, model), BF16),
            ],
        )
        return add(keep, peer(give))

    forward_out = sums((hid_0, hid_x, hid_y, hid_d), (wo, xo, yo, do), 0)
    input_grad = sums((pre_0, pre_x, pre_y, pre_d), (wi, xi, yi, di), 1)

    def share(own, x, y, dim):
        half = shape((width, span), F32)
        keep, give = run(split_kernel, (half, half), unit // 4, own, x, y)
        size = (span, n_rep * width) if dim else (n_rep * width, span)
        return run(
            functools.partial(join_kernel, dim), shape(size, F32), unit // 4,
            keep, peer(give),
        )

    down_grad = share(down_0, down_beside, down_across, 0)
    in_grad = share(into_0, into_beside, into_across, 1)
    return (forward_out, input_grad, in_grad, down_grad)


def solution(mesh):
    in_specs = (
        P(("blk", "rep"), None),
        P(("blk", "rep"), None),
        P(("blk", "rep"), None),
        P(None, "blk"),
        P("blk", None),
    )
    out_specs = (P(("blk", "rep"), None), P(("blk", "rep"), None), P("rep", "blk"), P("blk", "rep"))
    return jax.shard_map(window, mesh=mesh, in_specs=in_specs, out_specs=out_specs, check_vma=False)
```

```python
import functools

import jax
import jax.numpy as jnp
from jax import lax
from jax.experimental import pallas as pl
from jax.experimental.pallas import tpu as pltpu
from jax.sharding import PartitionSpec as P


TICKS = 4
SIDE = 2
ROOT = 0.7978845608028654
CUBE = 0.044715
F32, BF16 = jnp.float32, jnp.bfloat16


WEIGHT_KINDS = {"i": "A", "o": "A"}
GRAD_KINDS = {"d": "B", "n": "B"}


def routes(n_blk, n_rep):
    groups = n_blk // TICKS
    names = ("across", "across_but", "beside", "beside_but_last", "side", "third", "turn", "over")
    pairs = {name: [] for name in names}
    for blk in range(n_blk):
        group, place = blk // TICKS, blk % TICKS
        for rep in range(n_rep):
            source = blk * n_rep + rep

            def at(to, later=0):
                return (((group + later) % groups) * TICKS + to) * n_rep + rep

            def add(name, to, later=0):
                pairs[name].append((source, at(to, later)))

            add("across", place ^ SIDE, place ^ SIDE < place)
            add("beside", place ^ 1, place ^ 1 < place)
            if place < TICKS - 1:
                add("beside_but_last", place ^ 1, place ^ 1 < place)
            add("side", place ^ 1)
            if place == 0:
                add("third", SIDE)
                add("over", 1)
            if place != SIDE:
                add("across_but", place ^ SIDE, place ^ SIDE < place)
            add("turn", place ^ SIDE, (place == TICKS - 1) - (place == 0))
    return pairs


def back(pairs):
    return [(target, source) for source, target in pairs]


def mul(left, right, left_dim, right_dim):
    return lax.dot_general(
        left, right, (((left_dim,), (right_dim,)), ((), ())), preferred_element_type=F32
    )


def tanh_part(v):
    return jnp.tanh(ROOT * (v + CUBE * (v * v * v)))


def cut_kernel(dim, whole, part, sem):
    size = part.shape[dim]
    where = pl.ds(pl.multiple_of(lax.axis_index("rep") * size, size), size)
    copy = pltpu.make_async_copy(whole.at[:, where] if dim else whole.at[where, :], part, sem)
    copy.start()
    copy.wait()


def in_kernel(b0, b1, c0, c1, wi, down, slope, hid):
    for half, b in enumerate((b0, b1)):
        v = mul(b[...], wi[...], 1, 0)
        t = tanh_part(v)
        up = 0.5 * (1.0 + t)
        hid[half] = (v * up).astype(BF16)
        slope[half] = up + (0.5 * ROOT) * v * (1.0 - t * t) * (1.0 + (3.0 * CUBE) * (v * v))
    down[...] = (mul(hid[0], c0[...], 0, 0) + mul(hid[1], c1[...], 0, 0)).astype(down.dtype)


def out_kernel(b0, b1, c0, c1, wo, slope, into, pre):
    for half, c in enumerate((c0, c1)):
        pre[half] = (mul(c[...], wo[...], 1, 1) * slope[half]).astype(BF16)
    into[...] = (mul(pre[0], b0[...], 0, 0) + mul(pre[1], b1[...], 0, 0)).astype(into.dtype)


def fwd_kernel(f0, f1, wi, hid):
    for half, f in enumerate((f0, f1)):
        v = mul(f[...], wi[...], 1, 0)
        hid[half] = (v * (0.5 * (1.0 + tanh_part(v)))).astype(BF16)


def sum_kernel(dim, *refs):
    lefts, rights = refs[:TICKS], refs[TICKS : 2 * TICKS]
    give, keep, left, right = refs[2 * TICKS :]
    size = lefts[0].shape[2]
    for slot in range(TICKS):
        where = slice(slot * size, (slot + 1) * size)
        if dim:
            right[:, where] = rights[slot][...]
        else:
            right[where, :] = rights[slot][...]
        for half in range(2):
            left[half, :, where] = lefts[slot][half]
    give[...] = mul(left[1], right[...], 1, dim).astype(BF16)
    keep[...] = mul(left[0], right[...], 1, dim)


def add_kernel(a, b, out):
    out[...] = (a[...].astype(F32) + b[...].astype(F32)).astype(out.dtype)


def split_kernel(own, x, y, keep, give):
    rep, size = lax.axis_index("rep"), keep.shape[1]
    for out, at in ((give, 1 - rep), (keep, rep)):
        where = pl.ds(pl.multiple_of(at * size, size), size)
        total = own[:, where] + x[:, where].astype(F32) + y[:, where].astype(F32)
        out[...] = total.astype(out.dtype)


def join_kernel(dim, keep, got, out):
    rep, size = lax.axis_index("rep"), keep.shape[0]
    for part, at in ((keep, rep), (got, 1 - rep)):
        where = pl.ds(pl.multiple_of(at * size, size), size)
        if dim:
            out[:, where] = part[...].astype(F32).T
        else:
            out[where, :] = part[...].astype(F32)


def call(body, outs, flops, *args, scratch=(), far=False):
    vmem = pl.BlockSpec(memory_space=pltpu.VMEM)
    moved = sum(a.size * a.dtype.itemsize for a in args)
    return pl.pallas_call(
        body,
        out_shape=outs,
        in_specs=[pl.BlockSpec(memory_space=pltpu.HBM) if far else vmem] * len(args),
        out_specs=jax.tree.map(lambda _: vmem, outs),
        scratch_shapes=list(scratch),
        compiler_params=pltpu.CompilerParams(vmem_limit_bytes=14 << 20),
        cost_estimate=pl.CostEstimate(flops=flops, bytes_accessed=moved, transcendentals=0),
    )(*args)


def window(fwd_in, bwd_in, cotangent, w_in, w_out):
    axes = ("blk", "rep")
    n_blk, n_rep = lax.axis_size("blk"), lax.axis_size("rep")
    pairs = routes(n_blk, n_rep)
    width = w_in.shape[1] // n_rep
    rows, model = fwd_in.shape
    span = model // n_rep
    swap = [(0, 1), (1, 0)]
    unit = 2 * 2 * rows * model * width

    def move(value, pairs):
        return lax.ppermute(value, axes, pairs)

    def peer(value):
        return lax.ppermute(value, "rep", swap)

    shape = jax.ShapeDtypeStruct
    hidden = shape((2, rows, width), BF16)

    def run(body, outs, flops, *args, **rest):
        return call(body, outs, flops, *args, **rest)

    def in_part(a, kind):
        return run(
            in_kernel,
            (shape((width, model), kind), shape((2, rows, width), F32)),
            2 * unit,
            bwd_in, bwd_peer, cotangent, cot_peer, a,
            scratch=[pltpu.VMEM((2, rows, width), BF16)],
        )

    def out_part(b, slope, kind):
        return run(
            out_kernel,
            (shape((width, model), kind), hidden),
            2 * unit,
            bwd_in, bwd_peer, cotangent, cot_peer, b, slope,
        )

    def fwd_part(a):
        return run(fwd_kernel, hidden, unit, fwd_in, fwd_peer, a)

    def cut(whole, dim):
        size = (model, width) if dim else (width, model)
        return run(
            functools.partial(cut_kernel, dim), shape(size, BF16), unit // 4, whole,
            scratch=[pltpu.SemaphoreType.DMA], far=True,
        )

    def add(a, b):
        return run(add_kernel, shape(a.shape, BF16), unit // 4, a, b)

    def spread(label, weight):
        x = move(weight, pairs["beside"])
        y = move(weight, pairs["across"])
        if WEIGHT_KINDS[label] == "A":
            d = move(y, pairs["side"])
        else:
            d = move(x, pairs["turn"])
        return x, y, d

    wi, wo = cut(w_in, 1), cut(w_out, 0)
    xi, yi, di = spread("i", wi)
    xo, yo, do = spread("o", wo)
    bwd_peer, cot_peer, fwd_peer = peer(bwd_in), peer(cotangent), peer(fwd_in)

    down_0, slope_0 = in_part(wi, F32)
    into_0, pre_0 = out_part(wo, slope_0, F32)
    hid_0 = fwd_part(wi)
    down_y, slope_y = in_part(yi, BF16)
    into_y, pre_y = out_part(yo, slope_y, BF16)
    hid_y = fwd_part(yi)
    down_d, slope_d = in_part(di, BF16)
    into_d, pre_d = out_part(do, slope_d, BF16)
    hid_d = fwd_part(di)
    down_x, slope_x = in_part(xi, BF16)
    into_x, pre_x = out_part(xo, slope_x, BF16)
    hid_x = fwd_part(xi)

    def gather(label, g_x, g_y, g_d):
        rest = back(pairs["across"])
        if GRAD_KINDS[label] == "C":
            g_d = add(g_d, move(g_y, pairs["over"]))
            rest = back(pairs["across_but"])
        if GRAD_KINDS[label] == "A":
            g_y = add(g_y, move(g_d, back(pairs["side"])))
        else:
            g_x = add(g_x, move(g_d, back(pairs["turn"])))
        return (move(g_x, back(pairs["beside"])), move(g_y, rest))

    down_beside, down_across = gather("d", down_x, down_y, down_d)
    into_beside, into_across = gather("n", into_x, into_y, into_d)

    def sums(lefts, rights, dim):
        give, keep = run(
            functools.partial(sum_kernel, dim),
            (shape((rows, model), BF16), shape((rows, model), F32)),
            4 * unit, *lefts, *rights,
            scratch=[
                pltpu.VMEM((2, rows, TICKS * width), BF16),
                pltpu.VMEM((model, TICKS * width) if dim else (TICKS * width, model), BF16),
            ],
        )
        return add(keep, peer(give))

    forward_out = sums((hid_0, hid_x, hid_y, hid_d), (wo, xo, yo, do), 0)
    input_grad = sums((pre_0, pre_x, pre_y, pre_d), (wi, xi, yi, di), 1)

    def share(own, x, y, dim):
        half = shape((width, span), F32)
        sent = shape((width, span), BF16)
        keep, give = run(split_kernel, (half, sent), unit // 4, own, x, y)
        size = (span, n_rep * width) if dim else (n_rep * width, span)
        return run(
            functools.partial(join_kernel, dim), shape(size, F32), unit // 4,
            keep, peer(give),
        )

    down_grad = share(down_0, down_beside, down_across, 0)
    in_grad = share(into_0, into_beside, into_across, 1)
    return (forward_out, input_grad, in_grad, down_grad)


def solution(mesh):
    in_specs = (
        P(("blk", "rep"), None),
        P(("blk", "rep"), None),
        P(("blk", "rep"), None),
        P(None, "blk"),
        P("blk", None),
    )
    out_specs = (P(("blk", "rep"), None), P(("blk", "rep"), None), P("rep", "blk"), P("blk", "rep"))
    return jax.shard_map(window, mesh=mesh, in_specs=in_specs, out_specs=out_specs, check_vma=False)
```
